32 devices in a mesh: leaf: 8 (over z, x), rhs: 4 (over y, core).
Axes of the slice: x: 2, y: 2, z: 4, core: 2. Of those that a mesh axis runs over, the one named last changes fastest.
Arguments:
- right_sides: bfloat16 [8192, 4096], P('leaf', 'rhs'), may hold values from -6 to 6
- leaf_inverse: bfloat16 [8192, 1024], P(('leaf', 'rhs')), may hold values from -0.1875 to 0.1875
- project_factors: bfloat16 [3, 8192, 128], P(None, 'leaf'), may hold values from -0.1875 to 0.1875
- correct_factors: bfloat16 [3, 8192, 128], P(None, 'leaf'), may hold values from -0.5 to 0.5
- coupling_first: bfloat16 [4, 256, 256], P(None, 'rhs'), may hold values from -0.375 to 0.375
- coupling_second: bfloat16 [2, 256, 256], P(None, 'rhs'), may hold values from -0.375 to 0.375
- coupling_third: bfloat16 [1, 256, 256], P(None, 'rhs'), may hold values from -0.375 to 0.375
Outputs:
- solution: bfloat16 [8192, 4096], P('leaf', 'rhs')
The draws below stay inside these ranges and needn't reach their ends.
All inputs are finite; a program needn't handle non-finite values.
Results may differ from the reference program's by a relative error of at most 0.014.
Values may be sent and summed in bfloat16 or wider, within the bound.
A program may use at most 64 MiB of HBM per device.

```python
import jax
import jax.numpy as jnp
from jax import lax

LEAF = 1024
R = 128
LEVELS = 3
ORDER = 8192
COLS = 4096
N_LEAF = 8


def block_levels(key, dims, split, low, high):
    loudness, own = 1.0, jax.random.fold_in(key, 6)
    for axis_at, blocks in split:
        draws = jnp.exp(jax.random.uniform(jax.random.fold_in(own, axis_at), (blocks,), jnp.float32, low / len(split), high / len(split)))
        loudness = loudness * jnp.repeat(draws, dims[axis_at] // blocks).reshape([-1 if axis == axis_at else 1 for axis in range(len(dims))])
    return loudness


def normal_values(key, shape, spread, reach, shards=(), dtype=jnp.bfloat16):
    result = jax.random.normal(key, shape, jnp.float32) * spread
    if len(shards) > 0:
        result = block_levels(key, shape, shards, -0.22, 0.18) * result
    return jnp.clip(result, min=-reach, max=reach).astype(dtype)


def setup_inputs(seed: int = 0) -> dict:
    key_of = jax.random.split(jax.random.key(seed), 8)
    right_sides = normal_values(key_of[0], (ORDER, COLS), 1.0, 6.0, ((0, 8), (1, 4)))
    leaf_inverse = normal_values(key_of[1], (ORDER, LEAF), LEAF ** -0.5, 0.1875, ((0, 32),))
    project_factors = normal_values(key_of[2], (LEVELS, ORDER, R), LEAF ** -0.5, 0.1875, ((1, 8),))
    correct_factors = normal_values(key_of[3], (LEVELS, ORDER, R), R ** -0.5, 0.5, ((1, 8),))
    coupling_first = normal_values(key_of[4], (N_LEAF // 2, 2 * R, 2 * R), (2 * R) ** -0.5, 0.375, ((1, 4),))
    coupling_second = normal_values(key_of[5], (N_LEAF // 4, 2 * R, 2 * R), (2 * R) ** -0.5, 0.375, ((1, 4),))
    coupling_third = normal_values(key_of[6], (N_LEAF // 8, 2 * R, 2 * R), (2 * R) ** -0.5, 0.375, ((1, 4),))
    return dict(right_sides=right_sides, leaf_inverse=leaf_inverse, project_factors=project_factors, correct_factors=correct_factors, coupling_first=coupling_first, coupling_second=coupling_second, coupling_third=coupling_third)


def leaf_products(left, right):
    return lax.map(lambda pair: jnp.dot(pair[0], pair[1], preferred_element_type=jnp.float32), (left, right))


def reference(right_sides, leaf_inverse, project_factors, correct_factors, coupling_first, coupling_second, coupling_third):
    count = ORDER // LEAF
    blocks = right_sides.reshape(count, LEAF, COLS)
    inverse = leaf_inverse.reshape(count, LEAF, LEAF)
    start = leaf_products(inverse, blocks).astype(jnp.bfloat16)
    current = start.astype(jnp.float32)
    tables = (coupling_first, coupling_second, coupling_third)
    for level in range(LEVELS):
        rounded = current.astype(jnp.bfloat16)
        factors = project_factors[level].reshape(count, LEAF, R)
        terms = lax.map(lambda pair: jnp.dot(pair[0].T, pair[1], preferred_element_type=jnp.float32), (factors, rounded))
        group = 2 ** level
        projection = jnp.sum(terms.reshape(count // group, group, R, COLS), axis=1).astype(jnp.bfloat16)
        nodes = count // (2 * group)
        stacked = projection.reshape(nodes, 2 * R, COLS)
        answer = leaf_products(tables[level], stacked).astype(jnp.bfloat16)
        children = answer.reshape(2 * nodes, R, COLS)
        per_leaf = jnp.repeat(children, group, axis=0)
        left = correct_factors[level].reshape(count, LEAF, R)
        current = current - leaf_products(left, per_leaf)
    return current.reshape(ORDER, COLS).astype(jnp.bfloat16)
```

```python
import functools

import jax
import jax.numpy as jnp
from jax import lax
from jax.experimental import pallas as pl
from jax.experimental.pallas import tpu as pltpu
from jax.sharding import PartitionSpec as P

LEVELS = 3
CHUNKS = 4
BF = jnp.bfloat16
F32 = jnp.float32


def mm(a, b):
    return jnp.dot(a, b, preferred_element_type=F32)


def mmt(a, b):
    return lax.dot_general(a, b, (((0,), (0,)), ((), ())), preferred_element_type=F32)


def bit_of(index, stride):
    return lax.rem(lax.div(index, stride), 2)


def flip(index, stride):
    return index + stride * (1 - 2 * bit_of(index, stride))


def kernel(
    b_hbm, a_hbm, p_hbm, c_hbm, w0_hbm, w1_hbm, w2_hbm, out_hbm,
    b_v, a_v, p_v, c_v, w_v, g_v, qf, q_s, q_r, q_v,
    p0_s, p0_r, p1f, p1_s, p1_r, s1_s, s1_r, p2f, p2_s, p2_r,
    s2_s, s2_r, t2_s, t2_r, a_cat, start, out_v,
    lsem, osem, ssem, rsem,
):
    i = lax.axis_index("leaf")
    r = lax.axis_index("rhs")
    blk = a_hbm.shape[0]
    depth = a_hbm.shape[1]
    rows = b_hbm.shape[0]
    cols = b_hbm.shape[1]
    rank = p_hbm.shape[2]
    cw = cols // CHUNKS
    half = depth // 2
    mate = {"rhs": flip(r, 1)}
    across = {"rhs": flip(r, 2)}
    sib = {"leaf": flip(i, 1)}
    near = {"leaf": flip(i, 2)}
    far = {"leaf": flip(i, 4)}
    sides = [bit_of(i, 1), bit_of(i, 2), bit_of(i, 4)]
    core = bit_of(r, 1)
    chip = bit_of(r, 2)

    count = [0]
    copies = []

    def send(src, dst, to):
        k = count[0]
        count[0] += 1
        copy = pltpu.make_async_remote_copy(
            src_ref=src, dst_ref=dst, send_sem=ssem.at[k], recv_sem=rsem.at[k],
            device_id=to, device_id_type=pl.DeviceIdType.MESH,
        )
        copy.start()
        copies.append(copy)
        return copy

    nloc = [0]

    def fetch(src, dst):
        copy = pltpu.make_async_copy(src, dst, lsem.at[nloc[0]])
        nloc[0] += 1
        copy.start()
        return copy

    def block(which):
        return pl.ds(pl.multiple_of(which * blk, blk), blk)

    la = fetch(a_hbm, a_v.at[block(r), :])
    lw = [
        fetch(w_hbm.at[lax.div(i, 2 << level)], w_v.at[level, r])
        for level, w_hbm in enumerate((w0_hbm, w1_hbm, w2_hbm))
    ]
    lp = [fetch(p_hbm.at[l], p_v.at[:, pl.ds(l * rank, rank)]) for l in range(LEVELS)]
    lc = [fetch(c_hbm.at[l], c_v.at[:, pl.ds(l * rank, rank)]) for l in range(LEVELS)]
    lb = fetch(b_hbm, b_v)

    barrier = pltpu.get_barrier_semaphore()
    for to in (mate, across, sib, near, far):
        pl.semaphore_signal(barrier, inc=1, device_id=to, device_id_type=pl.DeviceIdType.MESH)
    pl.semaphore_wait(barrier, 5)

    la.wait()
    a_mate = send(a_v.at[block(r), :], a_v.at[block(r), :], mate)
    for copy in lw:
        copy.wait()
    w_across = send(w_v.at[:, r], w_v.at[:, r], across)
    w_mate = send(w_v.at[:, r], w_v.at[:, r], mate)
    for copy in lp:
        copy.wait()
    for copy in lc:
        copy.wait()
    a_mate.wait_recv()
    pair_rows = pl.ds(pl.multiple_of(chip * 2 * blk, 2 * blk), 2 * blk)
    half_cols = pl.ds(pl.multiple_of(core * half, half), half)
    q_across = []
    for l in range(LEVELS):
        part = mmt(p_v[pair_rows, pl.ds(l * rank, rank)], a_v[pair_rows, half_cols])
        qf[l] = part
        q_s[l] = part.astype(BF)
        q_across.append(send(q_s.at[l], q_r.at[l], across))
    pieces = 4
    piece = blk // pieces

    def piece_rows(which, k):
        return pl.ds(pl.multiple_of(which * blk + k * piece, piece), piece)

    a_across = [
        send(a_v.at[piece_rows(r, k), :], a_v.at[piece_rows(r, k), :], across)
        for k in range(pieces)
    ]
    for n, (l, k) in enumerate(((1, 0), (2, 0), (2, 1))):
        g_v[n] = mmt(p_v[:, pl.ds(l * rank, rank)], c_v[:, pl.ds(k * rank, rank)]).astype(BF)
    w_across.wait_recv()
    w_relay = send(w_v.at[:, flip(r, 2)], w_v.at[:, flip(r, 2)], mate)
    lb.wait()

    def finish_q(l):
        q_across[l].wait_recv()
        q_v[l, core] = (qf[l] + q_r[l].astype(F32)).astype(BF)
        return send(q_v.at[l, core], q_v.at[l, core], mate)

    def project(l, c):
        own = pl.ds(c * cw, cw)
        return mm(q_v[l, 0], b_v[pl.ds(0, half), own]) + mm(q_v[l, 1], b_v[pl.ds(half, half), own])

    def start_rows(which):
        for c in range(CHUNKS):
            own = pl.ds(c * cw, cw)
            start[block(which), own] = mm(a_v[block(which), :], b_v[:, own]).astype(BF)

    def weight(l, other):
        row = pl.ds(pl.multiple_of(sides[l] * 2, 2), 2)
        column = (1 - sides[l]) if other else sides[l]
        lanes = pl.ds(pl.multiple_of(column * rank, rank), rank)
        return w_v[l, row, :, lanes].reshape(rank, rank)

    q_mate = [finish_q(0)]
    q_mate[0].wait_recv()
    x0 = []
    for c in range(CHUNKS):
        p0_s[c] = project(0, c).astype(BF)
        x0.append(send(p0_s.at[c], p0_r.at[c], sib))
    q_mate.append(finish_q(1))
    start_rows(r)
    q_mate[1].wait_recv()
    for c in range(CHUNKS):
        p1f[c] = project(1, c)
    w_mate.wait_recv()
    w_relay.wait_recv()
    x1 = []
    for c in range(CHUNKS):
        x0[c].wait_recv()
        a0 = (mm(weight(0, False), p0_s[c]) + mm(weight(0, True), p0_r[c])).astype(BF)
        a_cat[c, pl.ds(0, rank), :] = a0
        part = p1f[c] - mm(g_v[0], a0)
        p1f[c] = part
        p1_s[c] = part.astype(BF)
        x1.append(send(p1_s.at[c], p1_r.at[c], sib))
    q_mate.append(finish_q(2))
    start_rows(flip(r, 1))
    q_mate[2].wait_recv()
    for c in range(CHUNKS):
        p2f[c] = project(2, c) - mm(g_v[1], a_cat[c, pl.ds(0, rank), :])
    z1 = []
    relay = []

    def relay_piece(k):
        a_across[k].wait_recv()
        where = piece_rows(flip(r, 2), k)
        relay.append(send(a_v.at[where, :], a_v.at[where, :], mate))

    for c in range(CHUNKS):
        x1[c].wait_recv()
        s1_s[c] = (p1f[c] + p1_r[c].astype(F32)).astype(BF)
        z1.append(send(s1_s.at[c], s1_r.at[c], near))
    x2 = []
    for c in range(CHUNKS):
        z1[c].wait_recv()
        a1 = (mm(weight(1, False), s1_s[c]) + mm(weight(1, True), s1_r[c])).astype(BF)
        a_cat[c, pl.ds(rank, rank), :] = a1
        part = p2f[c] - mm(g_v[2], a1)
        p2f[c] = part
        p2_s[c] = part.astype(BF)
        x2.append(send(p2_s.at[c], p2_r.at[c], sib))
    for k in range(pieces):
        relay_piece(k)
    n1 = []
    for c in range(CHUNKS):
        x2[c].wait_recv()
        p2f[c] = p2f[c] + p2_r[c].astype(F32)
        if c % 2 == 1:
            j = c // 2
            s2_s[j] = p2f[2 * j + 1 - sides[1]].astype(BF)
            n1.append(send(s2_s.at[j], s2_r.at[j], near))
    start_rows(flip(r, 2))
    f1 = []
    for j in range(CHUNKS // 2):
        n1[j].wait_recv()
        t2_s[j] = (p2f[2 * j + sides[1]] + s2_r[j].astype(F32)).astype(BF)
        f1.append(send(t2_s.at[j], t2_r.at[j], far))
    for copy in relay:
        copy.wait_recv()
    start_rows(flip(flip(r, 2), 1))
    n2 = []
    for j in range(CHUNKS // 2):
        f1[j].wait_recv()
        mine = 2 * j + sides[1]
        where = pl.ds(2 * rank, rank)
        a_cat[mine, where, :] = (
            mm(weight(2, False), t2_s[j]) + mm(weight(2, True), t2_r[j])
        ).astype(BF)
        n2.append(send(a_cat.at[mine, where, :], a_cat.at[mine, where, :], near))
    outs = []
    for c in range(CHUNKS):
        if c % 2 == 0:
            n2[c // 2].wait_recv()
        own = pl.ds(c * cw, cw)
        for n in range(4):
            band = pl.ds(n * (rows // 4), rows // 4)
            out_v[band, own] = (start[band, own].astype(F32) - mm(c_v[band, :], a_cat[c])).astype(BF)
        copy = pltpu.make_async_copy(out_v.at[:, own], out_hbm.at[:, own], osem.at[c])
        copy.start()
        outs.append(copy)
    for copy in copies:
        copy.wait_send()
    for copy in outs:
        copy.wait()


def local(right_sides, leaf_inverse, project_factors, correct_factors, *couplings):
    rows, cols = right_sides.shape
    blk, depth = leaf_inverse.shape
    levels, _, rank = project_factors.shape
    parts = lax.axis_size("rhs")
    cw = cols // CHUNKS
    full = lambda dtype: pltpu.VMEM((CHUNKS, rank, cw), dtype)
    part = lambda dtype: pltpu.VMEM((CHUNKS // 2, rank, cw), dtype)
    copies = 64
    any_spec = pl.BlockSpec(memory_space=pl.ANY)
    return pl.pallas_call(
        kernel,
        out_shape=jax.ShapeDtypeStruct((rows, cols), BF),
        in_specs=[any_spec] * 7,
        out_specs=any_spec,
        scratch_shapes=[
            pltpu.VMEM((rows, cols), BF),
            pltpu.VMEM((rows, depth), BF),
            pltpu.VMEM((rows, levels * rank), BF),
            pltpu.VMEM((rows, levels * rank), BF),
            pltpu.VMEM((levels, parts) + couplings[0].shape[1:], BF),
            pltpu.VMEM((3, rank, rank), BF),
            pltpu.VMEM((levels, rank, depth // 2), F32),
            pltpu.VMEM((levels, rank, depth // 2), BF),
            pltpu.VMEM((levels, rank, depth // 2), BF),
            pltpu.VMEM((levels, 2, rank, depth // 2), BF),
            full(BF), full(BF), full(F32), full(BF), full(BF), full(BF), full(BF),
            full(F32), full(BF), full(BF),
            part(BF), part(BF), part(BF), part(BF),
            pltpu.VMEM((CHUNKS, levels * rank, cw), BF),
            pltpu.VMEM((rows, cols), BF),
            pltpu.VMEM((rows, cols), BF),
            pltpu.SemaphoreType.DMA((16,)),
            pltpu.SemaphoreType.DMA((CHUNKS,)),
            pltpu.SemaphoreType.DMA((copies,)),
            pltpu.SemaphoreType.DMA((copies,)),
        ],
        compiler_params=pltpu.CompilerParams(
            collective_id=0, has_side_effects=True, vmem_limit_bytes=48 * 1024 * 1024
        ),
    )(right_sides, leaf_inverse, project_factors, correct_factors, *couplings)


def solution(mesh):
    in_specs = (
        P("leaf", "rhs"),
        P(("leaf", "rhs"), None),
        P(None, "leaf", None),
        P(None, "leaf", None),
        P(None, "rhs", None),
        P(None, "rhs", None),
        P(None, "rhs", None),
    )
    out_specs = P("leaf", "rhs")
    return jax.shard_map(local, mesh=mesh, in_specs=in_specs, out_specs=out_specs, check_vma=False)
```

```python
import functools

import jax
import jax.numpy as jnp
from jax import lax
from jax.experimental import pallas as pl
from jax.experimental.pallas import tpu as pltpu
from jax.sharding import PartitionSpec as P

LEVELS = 3
CHUNKS = 4
BF = jnp.bfloat16
F32 = jnp.float32


def mm(a, b):
    return jnp.dot(a, b, preferred_element_type=F32)


def mmt(a, b):
    return lax.dot_general(a, b, (((0,), (0,)), ((), ())), preferred_element_type=F32)


def bit_of(index, stride):
    return lax.rem(lax.div(index, stride), 2)


def flip(index, stride):
    return index + stride * (1 - 2 * bit_of(index, stride))


def kernel(
    b_hbm, a_hbm, p_hbm, c_hbm, w0_hbm, w1_hbm, w2_hbm, out_v,
    b_v, a_v, p_v, c_v, w_v, g_v, qf, q_s, q_r, q_v,
    p0_s, p0_r, p1f, p1_s, p1_r, s1_s, s1_r, p2f, p2_s, p2_r,
    s2_s, s2_r, t2_s, t2_r, a_cat, start,
    lsem, ssem, rsem,
):
    i = lax.axis_index("leaf")
    r = lax.axis_index("rhs")
    blk = a_hbm.shape[0]
    depth = a_hbm.shape[1]
    rows = b_hbm.shape[0]
    cols = b_hbm.shape[1]
    rank = p_hbm.shape[2]
    cw = cols // CHUNKS
    half = depth // 2
    mate = {"rhs": flip(r, 1)}
    across = {"rhs": flip(r, 2)}
    sib = {"leaf": flip(i, 1)}
    near = {"leaf": flip(i, 2)}
    far = {"leaf": flip(i, 4)}
    sides = [bit_of(i, 1), bit_of(i, 2), bit_of(i, 4)]
    core = bit_of(r, 1)
    chip = bit_of(r, 2)

    count = [0]
    copies = []

    def send(src, dst, to):
        k = count[0]
        count[0] += 1
        copy = pltpu.make_async_remote_copy(
            src_ref=src, dst_ref=dst, send_sem=ssem.at[k], recv_sem=rsem.at[k],
            device_id=to, device_id_type=pl.DeviceIdType.MESH,
        )
        copy.start()
        copies.append(copy)
        return copy

    nloc = [0]

    def fetch(src, dst):
        copy = pltpu.make_async_copy(src, dst, lsem.at[nloc[0]])
        nloc[0] += 1
        copy.start()
        return copy

    def block(which):
        return pl.ds(pl.multiple_of(which * blk, blk), blk)

    la = fetch(a_hbm, a_v.at[block(r), :])
    lw = [
        fetch(w_hbm.at[lax.div(i, 2 << level)], w_v.at[level, r])
        for level, w_hbm in enumerate((w0_hbm, w1_hbm, w2_hbm))
    ]
    lp = [fetch(p_hbm.at[l], p_v.at[:, pl.ds(l * rank, rank)]) for l in range(LEVELS)]
    lc = [fetch(c_hbm.at[l], c_v.at[:, pl.ds(l * rank, rank)]) for l in range(LEVELS)]
    lb = fetch(b_hbm, b_v)

    barrier = pltpu.get_barrier_semaphore()
    for to in (mate, across, sib, near, far):
        pl.semaphore_signal(barrier, inc=1, device_id=to, device_id_type=pl.DeviceIdType.MESH)
    pl.semaphore_wait(barrier, 5)

    la.wait()
    a_mate = send(a_v.at[block(r), :], a_v.at[block(r), :], mate)
    for copy in lw:
        copy.wait()
    w_across = send(w_v.at[:, r], w_v.at[:, r], across)
    w_mate = send(w_v.at[:, r], w_v.at[:, r], mate)
    for copy in lp:
        copy.wait()
    for copy in lc:
        copy.wait()
    a_mate.wait_recv()
    pair_rows = pl.ds(pl.multiple_of(chip * 2 * blk, 2 * blk), 2 * blk)
    half_cols = pl.ds(pl.multiple_of(core * half, half), half)
    q_across = []
    for l in range(LEVELS):
        part = mmt(p_v[pair_rows, pl.ds(l * rank, rank)], a_v[pair_rows, half_cols])
        qf[l] = part
        q_s[l] = part.astype(BF)
        q_across.append(send(q_s.at[l], q_r.at[l], across))
    pieces = 4
    piece = blk // pieces

    def piece_rows(which, k):
        return pl.ds(pl.multiple_of(which * blk + k * piece, piece), piece)

    a_across = [
        send(a_v.at[piece_rows(r, k), :], a_v.at[piece_rows(r, k), :], across)
        for k in range(pieces)
    ]
    for n, (l, k) in enumerate(((1, 0), (2, 0), (2, 1))):
        g_v[n] = mmt(p_v[:, pl.ds(l * rank, rank)], c_v[:, pl.ds(k * rank, rank)]).astype(BF)
    w_across.wait_recv()
    w_relay = send(w_v.at[:, flip(r, 2)], w_v.at[:, flip(r, 2)], mate)
    lb.wait()

    def finish_q(l):
        q_across[l].wait_recv()
        q_v[l, core] = (qf[l] + q_r[l].astype(F32)).astype(BF)
        return send(q_v.at[l, core], q_v.at[l, core], mate)

    def project(l, c):
        own = pl.ds(c * cw, cw)
        return mm(q_v[l, 0], b_v[pl.ds(0, half), own]) + mm(q_v[l, 1], b_v[pl.ds(half, half), own])

    def start_rows(which):
        for c in range(CHUNKS):
            own = pl.ds(c * cw, cw)
            start[block(which), own] = mm(a_v[block(which), :], b_v[:, own]).astype(BF)

    def weight(l, other):
        row = pl.ds(pl.multiple_of(sides[l] * 2, 2), 2)
        column = (1 - sides[l]) if other else sides[l]
        lanes = pl.ds(pl.multiple_of(column * rank, rank), rank)
        return w_v[l, row, :, lanes].reshape(rank, rank)

    q_mate = [finish_q(0)]
    q_mate[0].wait_recv()
    x0 = []
    for c in range(CHUNKS):
        p0_s[c] = project(0, c).astype(BF)
        x0.append(send(p0_s.at[c], p0_r.at[c], sib))
    q_mate.append(finish_q(1))
    start_rows(r)
    q_mate[1].wait_recv()
    for c in range(CHUNKS):
        p1f[c] = project(1, c)
    w_mate.wait_recv()
    w_relay.wait_recv()
    x1 = []
    for c in range(CHUNKS):
        x0[c].wait_recv()
        a0 = (mm(weight(0, False), p0_s[c]) + mm(weight(0, True), p0_r[c])).astype(BF)
        a_cat[c, pl.ds(0, rank), :] = a0
        part = p1f[c] - mm(g_v[0], a0)
        p1f[c] = part
        p1_s[c] = part.astype(BF)
        x1.append(send(p1_s.at[c], p1_r.at[c], sib))
    q_mate.append(finish_q(2))
    start_rows(flip(r, 1))
    q_mate[2].wait_recv()
    for c in range(CHUNKS):
        p2f[c] = project(2, c) - mm(g_v[1], a_cat[c, pl.ds(0, rank), :])
    z1 = []
    relay = []

    def relay_piece(k):
        a_across[k].wait_recv()
        where = piece_rows(flip(r, 2), k)
        relay.append(send(a_v.at[where, :], a_v.at[where, :], mate))

    for c in range(CHUNKS):
        x1[c].wait_recv()
        s1_s[c] = (p1f[c] + p1_r[c].astype(F32)).astype(BF)
        z1.append(send(s1_s.at[c], s1_r.at[c], near))
    x2 = []
    for c in range(CHUNKS):
        z1[c].wait_recv()
        a1 = (mm(weight(1, False), s1_s[c]) + mm(weight(1, True), s1_r[c])).astype(BF)
        a_cat[c, pl.ds(rank, rank), :] = a1
        part = p2f[c] - mm(g_v[2], a1)
        p2f[c] = part
        p2_s[c] = part.astype(BF)
        x2.append(send(p2_s.at[c], p2_r.at[c], sib))
    for k in range(pieces):
        relay_piece(k)
    n1 = []
    for c in range(CHUNKS):
        x2[c].wait_recv()
        p2f[c] = p2f[c] + p2_r[c].astype(F32)
        if c % 2 == 1:
            j = c // 2
            s2_s[j] = p2f[2 * j + 1 - sides[1]].astype(BF)
            n1.append(send(s2_s.at[j], s2_r.at[j], near))
    start_rows(flip(r, 2))
    f1 = []
    for j in range(CHUNKS // 2):
        n1[j].wait_recv()
        t2_s[j] = (p2f[2 * j + sides[1]] + s2_r[j].astype(F32)).astype(BF)
        f1.append(send(t2_s.at[j], t2_r.at[j], far))
    for copy in relay:
        copy.wait_recv()
    start_rows(flip(flip(r, 2), 1))
    n2 = []
    for j in range(CHUNKS // 2):
        f1[j].wait_recv()
        mine = 2 * j + sides[1]
        where = pl.ds(2 * rank, rank)
        a_cat[mine, where, :] = (
            mm(weight(2, False), t2_s[j]) + mm(weight(2, True), t2_r[j])
        ).astype(BF)
        n2.append(send(a_cat.at[mine, where, :], a_cat.at[mine, where, :], near))
    for c in range(CHUNKS):
        if c % 2 == 0:
            n2[c // 2].wait_recv()
        own = pl.ds(c * cw, cw)
        for n in range(4):
            band = pl.ds(n * (rows // 4), rows // 4)
            out_v[band, own] = (start[band, own].astype(F32) - mm(c_v[band, :], a_cat[c])).astype(BF)
    for copy in copies:
        copy.wait_send()


def local(right_sides, leaf_inverse, project_factors, correct_factors, *couplings):
    rows, cols = right_sides.shape
    blk, depth = leaf_inverse.shape
    levels, _, rank = project_factors.shape
    parts = lax.axis_size("rhs")
    cw = cols // CHUNKS
    full = lambda dtype: pltpu.VMEM((CHUNKS, rank, cw), dtype)
    part = lambda dtype: pltpu.VMEM((CHUNKS // 2, rank, cw), dtype)
    copies = 64
    any_spec = pl.BlockSpec(memory_space=pltpu.HBM)
    return pl.pallas_call(
        kernel,
        out_shape=jax.ShapeDtypeStruct((rows, cols), BF),
        in_specs=[any_spec] * 7,
        out_specs=pl.BlockSpec(memory_space=pltpu.VMEM),
        scratch_shapes=[
            pltpu.VMEM((rows, cols), BF),
            pltpu.VMEM((rows, depth), BF),
            pltpu.VMEM((rows, levels * rank), BF),
            pltpu.VMEM((rows, levels * rank), BF),
            pltpu.VMEM((levels, parts) + couplings[0].shape[1:], BF),
            pltpu.VMEM((3, rank, rank), BF),
            pltpu.VMEM((levels, rank, depth // 2), F32),
            pltpu.VMEM((levels, rank, depth // 2), BF),
            pltpu.VMEM((levels, rank, depth // 2), BF),
            pltpu.VMEM((levels, 2, rank, depth // 2), BF),
            full(BF), full(BF), full(F32), full(BF), full(BF), full(BF), full(BF),
            full(F32), full(BF), full(BF),
            part(BF), part(BF), part(BF), part(BF),
            pltpu.VMEM((CHUNKS, levels * rank, cw), BF),
            pltpu.VMEM((rows, cols), BF),
            pltpu.SemaphoreType.DMA((16,)),
            pltpu.SemaphoreType.DMA((copies,)),
            pltpu.SemaphoreType.DMA((copies,)),
        ],
        compiler_params=pltpu.CompilerParams(
            collective_id=0, has_side_effects=True, vmem_limit_bytes=48 * 1024 * 1024
        ),
    )(*(
        pltpu.with_memory_space_constraint(x, pltpu.HBM)
        for x in (right_sides, leaf_inverse, project_factors, correct_factors, *couplings)
    ))


def solution(mesh):
    in_specs = (
        P("leaf", "rhs"),
        P(("leaf", "rhs"), None),
        P(None, "leaf", None),
        P(None, "leaf", None),
        P(None, "rhs", None),
        P(None, "rhs", None),
        P(None, "rhs", None),
    )
    out_specs = P("leaf", "rhs")
    return jax.shard_map(local, mesh=mesh, in_specs=in_specs, out_specs=out_specs, check_vma=False)
```

```python
import functools

import jax
import jax.numpy as jnp
from jax import lax
from jax.experimental import pallas as pl
from jax.experimental.pallas import tpu as pltpu
from jax.sharding import PartitionSpec as P

LEVELS = 3
CHUNKS = 4
BF = jnp.bfloat16
F32 = jnp.float32


def mm(a, b):
    return jnp.dot(a, b, preferred_element_type=F32)


def bit_of(index, stride):
    return lax.rem(lax.div(index, stride), 2)


def flip(index, stride):
    return index + stride * (1 - 2 * bit_of(index, stride))


def kernel(
    b_hbm, a_hbm, p_hbm, c_hbm, w0_hbm, w1_hbm, w2_hbm, out_v,
    b_v, a_v, p_v, pt_v, c_v, w_v, g_v, qf, q_s, q_r, q_v,
    stack, p0f, p0_s, p0_r, p1f, p1_s, p1_r, s1_s, s1_r, p2f, p2_s, p2_r,
    s2_s, s2_r, t2_s, t2_r, a_cat, start,
    lsem, ssem, rsem,
):
    i = lax.axis_index("leaf")
    r = lax.axis_index("rhs")
    blk = a_hbm.shape[0]
    depth = a_hbm.shape[1]
    rows = b_hbm.shape[0]
    cols = b_hbm.shape[1]
    rank = p_hbm.shape[2]
    cw = cols // CHUNKS
    half = depth // 2
    mate = {"rhs": flip(r, 1)}
    across = {"rhs": flip(r, 2)}
    sib = {"leaf": flip(i, 1)}
    near = {"leaf": flip(i, 2)}
    far = {"leaf": flip(i, 4)}
    diag = {"leaf": flip(flip(i, 1), 2)}
    sides = [bit_of(i, 1), bit_of(i, 2), bit_of(i, 4)]
    core = bit_of(r, 1)
    chip = bit_of(r, 2)

    count = [0]
    copies = []

    def send(src, dst, to):
        k = count[0]
        count[0] += 1
        copy = pltpu.make_async_remote_copy(
            src_ref=src, dst_ref=dst, send_sem=ssem.at[k], recv_sem=rsem.at[k],
            device_id=to, device_id_type=pl.DeviceIdType.MESH,
        )
        copy.start()
        copies.append(copy)
        return copy

    nloc = [0]

    def fetch(src, dst):
        copy = pltpu.make_async_copy(src, dst, lsem.at[nloc[0]])
        nloc[0] += 1
        copy.start()
        return copy

    def block(which):
        return pl.ds(pl.multiple_of(which * blk, blk), blk)

    la = fetch(a_hbm, a_v.at[block(r), :])
    lw = [
        fetch(w_hbm.at[lax.div(i, 2 << level)], w_v.at[level, r])
        for level, w_hbm in enumerate((w0_hbm, w1_hbm, w2_hbm))
    ]
    lp = [fetch(p_hbm.at[l], p_v.at[:, pl.ds(l * rank, rank)]) for l in range(LEVELS)]
    lc = [fetch(c_hbm.at[l], c_v.at[:, pl.ds(l * rank, rank)]) for l in range(LEVELS)]
    lb = fetch(b_hbm, b_v)

    barrier = pltpu.get_barrier_semaphore()
    for to in (mate, across, sib, near, far, diag):
        pl.semaphore_signal(barrier, inc=1, device_id=to, device_id_type=pl.DeviceIdType.MESH)
    for l in range(LEVELS):
        lp[l].wait()
        pt_v[l] = p_v[:, pl.ds(l * rank, rank)].T
    pl.semaphore_wait(barrier, 6)

    la.wait()
    half_cols = pl.ds(pl.multiple_of(core * half, half), half)
    rest_cols = pl.ds(pl.multiple_of((1 - core) * half, half), half)
    a_mate = send(a_v.at[block(r), rest_cols], a_v.at[block(r), rest_cols], mate)
    a_mate2 = send(a_v.at[block(r), half_cols], a_v.at[block(r), half_cols], mate)
    for copy in lw:
        copy.wait()
    w_across = [send(w_v.at[0, r], w_v.at[0, r], across)]
    w_mate = send(w_v.at[:, r], w_v.at[:, r], mate)
    a_mate.wait_recv()
    pair_rows = pl.ds(pl.multiple_of(chip * 2 * blk, 2 * blk), 2 * blk)
    q_across = []
    for l in range(LEVELS):
        part = mm(pt_v[l, :, pair_rows], a_v[pair_rows, half_cols])
        qf[l] = part
        q_s[l] = part.astype(BF)
        q_across.append(send(q_s.at[l], q_r.at[l], across))
    for l in range(1, LEVELS):
        w_across.append(send(w_v.at[l, r], w_v.at[l, r], across))
    pieces = 4
    piece = blk // pieces

    def piece_rows(which, k):
        return pl.ds(pl.multiple_of(which * blk + k * piece, piece), piece)

    a_across = [
        send(a_v.at[piece_rows(r, k), :], a_v.at[piece_rows(r, k), :], across)
        for k in range(pieces)
    ]
    for copy in lc:
        copy.wait()
    own_lanes = pl.ds(pl.multiple_of(sides[0] * rank, rank), rank)
    g_send = []
    for n, (l, k) in enumerate(((1, 0), (2, 0), (2, 1))):
        g_v[n, :, own_lanes] = mm(pt_v[l], c_v[:, pl.ds(k * rank, rank)]).astype(BF)
        g_send.append(send(g_v.at[n, :, own_lanes], g_v.at[n, :, own_lanes], sib))

    def relay_w(l):
        w_across[l].wait_recv()
        w_relay.append(send(w_v.at[l, flip(r, 2)], w_v.at[l, flip(r, 2)], mate))

    w_relay = []
    relay_w(0)
    lb.wait()

    def finish_q(l):
        q_across[l].wait_recv()
        q_v[l, core] = (qf[l] + q_r[l].astype(F32)).astype(BF)
        return send(q_v.at[l, core], q_v.at[l, core], mate)

    def project(l, c):
        own = pl.ds(c * cw, cw)
        return mm(q_v[l, 0], b_v[pl.ds(0, half), own]) + mm(q_v[l, 1], b_v[pl.ds(half, half), own])

    def start_rows(which):
        for c in range(CHUNKS):
            own = pl.ds(c * cw, cw)
            start[block(which), own] = mm(a_v[block(which), :], b_v[:, own]).astype(BF)

    def weight(l, other):
        row = pl.ds(pl.multiple_of(sides[l] * 2, 2), 2)
        column = (1 - sides[l]) if other else sides[l]
        lanes = pl.ds(pl.multiple_of(column * rank, rank), rank)
        return w_v[l, row, :, lanes].reshape(rank, rank)

    hw = cw // 2
    keep = pl.ds(pl.multiple_of(sides[0] * hw, hw), hw)
    give = pl.ds(pl.multiple_of((1 - sides[0]) * hw, hw), hw)
    exchange = []
    for l, (f_v, s_v, r_v) in enumerate(((p0f, p0_s, p0_r), (p1f, p1_s, p1_r), (p2f, p2_s, p2_r))):
        copy = finish_q(l)
        if l == 2:
            a_mate2.wait_recv()
            start_rows(r)
        copy.wait_recv()
        sends = []
        for c in range(CHUNKS):
            part = project(l, c)
            if l > 0:
                f_v[c] = part
            if l < 2:
                s_v[c] = part.astype(BF)
            else:
                s_v[c] = f_v[c, :, give].astype(BF)
            sends.append(send(s_v.at[c], r_v.at[c], sib))
        exchange.append(sends)
    x0, x1, x2 = exchange
    w_mate.wait_recv()
    w_relay[0].wait_recv()
    for copy in g_send:
        copy.wait_recv()
    mine_rows = pl.ds(pl.multiple_of(sides[0] * rank, rank), rank)
    other_rows = pl.ds(pl.multiple_of((1 - sides[0]) * rank, rank), rank)
    node = w_v[0].reshape(2 * rank, 2 * rank)

    def first(c):
        x0[c].wait_recv()
        stack[c, mine_rows, :] = p0_s[c]
        stack[c, other_rows, :] = p0_r[c]
        both = mm(node, stack[c]).astype(BF)
        stack[c] = both
        a_cat[c, pl.ds(0, rank), :] = stack[c, mine_rows, :]
        p1f[c] = p1f[c] - mm(g_v[0], both)
        p2f[c, :, keep] = p2f[c, :, keep] - mm(g_v[1], stack[c, :, keep])

    z1 = []

    def second_sum(c):
        x1[c].wait_recv()
        s1_s[c] = (p1f[c] + p1_r[c].astype(F32)).astype(BF)
        z1.append(send(s1_s.at[c], s1_r.at[c], near))

    def second(c):
        z1[c].wait_recv()
        a1 = (mm(weight(1, False), s1_s[c]) + mm(weight(1, True), s1_r[c])).astype(BF)
        a_cat[c, pl.ds(rank, rank), :] = a1
        a1 = a_cat[c, pl.ds(rank, rank), keep]
        p2f[c, :, keep] = (
            p2f[c, :, keep] - mm(g_v[2, :, pl.ds(0, rank)], a1) - mm(g_v[2, :, pl.ds(rank, rank)], a1)
        )

    n1 = []

    def third_sum(c):
        x2[c].wait_recv()
        p2f[c, :, keep] = p2f[c, :, keep] + p2_r[c].astype(F32)
        if c % 2 == 1:
            j = c // 2
            s2_s[j] = p2f[2 * j + 1 - sides[1], :, keep].astype(BF)
            n1.append(send(s2_s.at[j], s2_r.at[j], near))

    f1 = []

    def third_far(j):
        n1[j].wait_recv()
        t2_s[j] = (p2f[2 * j + sides[1], :, keep] + s2_r[j].astype(F32)).astype(BF)
        f1.append(send(t2_s.at[j], t2_r.at[j], far))

    n2 = []

    def third(j):
        f1[j].wait_recv()
        mine = 2 * j + sides[1]
        where = pl.ds(2 * rank, rank)
        a_cat[mine, where, keep] = (
            mm(weight(2, False), t2_s[j]) + mm(weight(2, True), t2_r[j])
        ).astype(BF)
        spot = a_cat.at[mine, where, keep]
        n2.append([send(spot, spot, to) for to in (diag, sib, near)])

    relay = []

    def relay_piece(k):
        a_across[k].wait_recv()
        where = piece_rows(flip(r, 2), k)
        relay.append(send(a_v.at[where, :], a_v.at[where, :], mate))

    def finish(c):
        own = pl.ds(c * cw, cw)
        for n in range(4):
            band = pl.ds(n * (rows // 4), rows // 4)
            out_v[band, own] = (start[band, own].astype(F32) - mm(c_v[band, :], a_cat[c])).astype(BF)

    relay_w(1)
    relay_w(2)
    start_rows(flip(r, 1))
    for c in range(CHUNKS):
        first(c)
    for c in range(CHUNKS):
        second_sum(c)
        if c == 1:
            w_relay[1].wait_recv()
            w_relay[2].wait_recv()
    lag = CHUNKS // 2
    for c in range(lag):
        second(c)
    for c in range(CHUNKS):
        if c + lag < CHUNKS:
            second(c + lag)
        third_sum(c)
    for k in range(pieces):
        relay_piece(k)
    for j in range(CHUNKS // 2):
        third_far(j)
    start_rows(flip(r, 2))
    for copy in relay:
        copy.wait_recv()
    start_rows(flip(flip(r, 2), 1))
    for j in range(CHUNKS // 2):
        third(j)
    for j in range(CHUNKS // 2):
        for copy in n2[j]:
            copy.wait_recv()
        finish(2 * j)
        finish(2 * j + 1)
    for copy in copies:
        copy.wait_send()


def local(right_sides, leaf_inverse, project_factors, correct_factors, *couplings):
    rows, cols = right_sides.shape
    blk, depth = leaf_inverse.shape
    levels, _, rank = project_factors.shape
    parts = lax.axis_size("rhs")
    cw = cols // CHUNKS
    full = lambda dtype: pltpu.VMEM((CHUNKS, rank, cw), dtype)
    thin = lambda dtype: pltpu.VMEM((CHUNKS, rank, cw // 2), dtype)
    part = lambda dtype: pltpu.VMEM((CHUNKS // 2, rank, cw // 2), dtype)
    copies = 96
    any_spec = pl.BlockSpec(memory_space=pltpu.HBM)
    return pl.pallas_call(
        kernel,
        out_shape=jax.ShapeDtypeStruct((rows, cols), BF),
        in_specs=[any_spec] * 7,
        out_specs=pl.BlockSpec(memory_space=pltpu.VMEM),
        scratch_shapes=[
            pltpu.VMEM((rows, cols), BF),
            pltpu.VMEM((rows, depth), BF),
            pltpu.VMEM((rows, levels * rank), BF),
            pltpu.VMEM((levels, rank, rows), BF),
            pltpu.VMEM((rows, levels * rank), BF),
            pltpu.VMEM((levels, parts) + couplings[0].shape[1:], BF),
            pltpu.VMEM((3, rank, 2 * rank), BF),
            pltpu.VMEM((levels, rank, depth // 2), F32),
            pltpu.VMEM((levels, rank, depth // 2), BF),
            pltpu.VMEM((levels, rank, depth // 2), BF),
            pltpu.VMEM((levels, 2, rank, depth // 2), BF),
            pltpu.VMEM((CHUNKS, 2 * rank, cw), BF),
            full(F32), full(BF), full(BF), full(F32), full(BF), full(BF), full(BF), full(BF),
            full(F32), thin(BF), thin(BF),
            part(BF), part(BF), part(BF), part(BF),
            pltpu.VMEM((CHUNKS, levels * rank, cw), BF),
            pltpu.VMEM((rows, cols), BF),
            pltpu.SemaphoreType.DMA((16,)),
            pltpu.SemaphoreType.DMA((copies,)),
            pltpu.SemaphoreType.DMA((copies,)),
        ],
        compiler_params=pltpu.CompilerParams(
            collective_id=0, has_side_effects=True, vmem_limit_bytes=48 * 1024 * 1024
        ),
    )(*(
        pltpu.with_memory_space_constraint(x, pltpu.HBM)
        for x in (right_sides, leaf_inverse, project_factors, correct_factors, *couplings)
    ))


def solution(mesh):
    in_specs = (
        P("leaf", "rhs"),
        P(("leaf", "rhs"), None),
        P(None, "leaf", None),
        P(None, "leaf", None),
        P(None, "rhs", None),
        P(None, "rhs", None),
        P(None, "rhs", None),
    )
    out_specs = P("leaf", "rhs")
    return jax.shard_map(local, mesh=mesh, in_specs=in_specs, out_specs=out_specs, check_vma=False)
```

```python
import functools

import jax
import jax.numpy as jnp
from jax import lax
from jax.experimental import pallas as pl
from jax.experimental.pallas import tpu as pltpu
from jax.sharding import PartitionSpec as P

LEVELS = 3
CHUNKS = 4
BF = jnp.bfloat16
F32 = jnp.float32


def mm(a, b):
    return jnp.dot(a, b, preferred_element_type=F32)


def bit_of(index, stride):
    return lax.rem(lax.div(index, stride), 2)


def flip(index, stride):
    return index + stride * (1 - 2 * bit_of(index, stride))


def kernel(
    b_hbm, a_hbm, p_hbm, c_hbm, w0_hbm, w1_hbm, w2_hbm, out_v,
    b_v, a_v, p_v, pt_v, c_v, w_v, g_v, qf, q_s, q_r, q_v,
    stack, p0f, p0_s, p0_r, p1f, p1_s, p1_r, s1_s, s1_r, p2f, p2_s, p2_r,
    s2_s, s2_r, t2_s, t2_r, a_cat, start,
    lsem, ssem, rsem,
):
    i = lax.axis_index("leaf")
    r = lax.axis_index("rhs")
    blk = a_hbm.shape[0]
    depth = a_hbm.shape[1]
    rows = b_hbm.shape[0]
    cols = b_hbm.shape[1]
    rank = p_hbm.shape[2]
    cw = cols // CHUNKS
    half = depth // 2
    mate = {"rhs": flip(r, 1)}
    across = {"rhs": flip(r, 2)}
    sib = {"leaf": flip(i, 1)}
    near = {"leaf": flip(i, 2)}
    far = {"leaf": flip(i, 4)}
    diag = {"leaf": flip(flip(i, 1), 2)}
    sides = [bit_of(i, 1), bit_of(i, 2), bit_of(i, 4)]
    core = bit_of(r, 1)
    chip = bit_of(r, 2)

    count = [0]
    copies = []

    def send(src, dst, to):
        k = count[0]
        count[0] += 1
        copy = pltpu.make_async_remote_copy(
            src_ref=src, dst_ref=dst, send_sem=ssem.at[k], recv_sem=rsem.at[k],
            device_id=to, device_id_type=pl.DeviceIdType.MESH,
        )
        copy.start()
        copies.append(copy)
        return copy

    nloc = [0]

    def fetch(src, dst):
        copy = pltpu.make_async_copy(src, dst, lsem.at[nloc[0]])
        nloc[0] += 1
        copy.start()
        return copy

    def block(which):
        return pl.ds(pl.multiple_of(which * blk, blk), blk)

    la = fetch(a_hbm, a_v.at[block(r), :])
    lw = [
        fetch(w_hbm.at[lax.div(i, 2 << level)], w_v.at[level, r])
        for level, w_hbm in enumerate((w0_hbm, w1_hbm, w2_hbm))
    ]
    lp = [fetch(p_hbm.at[l], p_v.at[:, pl.ds(l * rank, rank)]) for l in range(LEVELS)]
    lc = [fetch(c_hbm.at[l], c_v.at[:, pl.ds(l * rank, rank)]) for l in range(LEVELS)]
    lb = fetch(b_hbm, b_v)

    barrier = pltpu.get_barrier_semaphore()
    for to in (mate, across, sib, near, far, diag):
        pl.semaphore_signal(barrier, inc=1, device_id=to, device_id_type=pl.DeviceIdType.MESH)
    lp[0].wait()
    pt_v[0] = p_v[:, pl.ds(0, rank)].T
    pl.semaphore_wait(barrier, 6)

    la.wait()
    half_cols = pl.ds(pl.multiple_of(core * half, half), half)
    rest_cols = pl.ds(pl.multiple_of((1 - core) * half, half), half)
    a_mate = send(a_v.at[block(r), rest_cols], a_v.at[block(r), rest_cols], mate)
    a_mate2 = send(a_v.at[block(r), half_cols], a_v.at[block(r), half_cols], mate)
    for copy in lw:
        copy.wait()
    w_across = [send(w_v.at[0, r], w_v.at[0, r], across)]
    w_mate = send(w_v.at[:, r], w_v.at[:, r], mate)
    a_mate.wait_recv()
    pair_rows = pl.ds(pl.multiple_of(chip * 2 * blk, 2 * blk), 2 * blk)
    q_across = []
    for l in range(LEVELS):
        if l > 0:
            lp[l].wait()
            pt_v[l] = p_v[:, pl.ds(l * rank, rank)].T
        part = mm(pt_v[l, :, pair_rows], a_v[pair_rows, half_cols])
        qf[l] = part
        q_s[l] = part.astype(BF)
        q_across.append(send(q_s.at[l], q_r.at[l], across))
    for l in range(1, LEVELS):
        w_across.append(send(w_v.at[l, r], w_v.at[l, r], across))
    pieces = 4
    piece = blk // pieces

    def piece_rows(which, k):
        return pl.ds(pl.multiple_of(which * blk + k * piece, piece), piece)

    a_across = [
        send(a_v.at[piece_rows(r, k), :], a_v.at[piece_rows(r, k), :], across)
        for k in range(pieces)
    ]
    for copy in lc:
        copy.wait()
    own_lanes = pl.ds(pl.multiple_of(sides[0] * rank, rank), rank)
    g_send = []
    for n, (l, k) in enumerate(((1, 0), (2, 0), (2, 1))):
        g_v[n, :, own_lanes] = mm(pt_v[l], c_v[:, pl.ds(k * rank, rank)]).astype(BF)
        g_send.append(send(g_v.at[n, :, own_lanes], g_v.at[n, :, own_lanes], sib))

    def relay_w(l):
        w_across[l].wait_recv()
        w_relay.append(send(w_v.at[l, flip(r, 2)], w_v.at[l, flip(r, 2)], mate))

    w_relay = []
    relay_w(0)
    lb.wait()

    def finish_q(l):
        q_across[l].wait_recv()
        q_v[l, core] = (qf[l] + q_r[l].astype(F32)).astype(BF)
        return send(q_v.at[l, core], q_v.at[l, core], mate)

    def project(l, c):
        own = pl.ds(c * cw, cw)
        return mm(q_v[l, 0], b_v[pl.ds(0, half), own]) + mm(q_v[l, 1], b_v[pl.ds(half, half), own])

    def start_rows(which):
        for c in range(CHUNKS):
            own = pl.ds(c * cw, cw)
            start[block(which), own] = mm(a_v[block(which), :], b_v[:, own]).astype(BF)

    def weight(l, other):
        row = pl.ds(pl.multiple_of(sides[l] * 2, 2), 2)
        column = (1 - sides[l]) if other else sides[l]
        lanes = pl.ds(pl.multiple_of(column * rank, rank), rank)
        return w_v[l, row, :, lanes].reshape(rank, rank)

    hw = cw // 2
    keep = pl.ds(pl.multiple_of(sides[0] * hw, hw), hw)
    give = pl.ds(pl.multiple_of((1 - sides[0]) * hw, hw), hw)
    exchange = []
    for l, (f_v, s_v, r_v) in enumerate(((p0f, p0_s, p0_r), (p1f, p1_s, p1_r), (p2f, p2_s, p2_r))):
        copy = finish_q(l)
        if l == 2:
            a_mate2.wait_recv()
            start_rows(r)
        copy.wait_recv()
        sends = []
        for c in range(CHUNKS):
            part = project(l, c)
            if l > 0:
                f_v[c] = part
            if l < 2:
                s_v[c] = part.astype(BF)
            else:
                s_v[c] = f_v[c, :, give].astype(BF)
            sends.append(send(s_v.at[c], r_v.at[c], sib))
        exchange.append(sends)
    x0, x1, x2 = exchange
    w_mate.wait_recv()
    w_relay[0].wait_recv()
    for copy in g_send:
        copy.wait_recv()
    mine_rows = pl.ds(pl.multiple_of(sides[0] * rank, rank), rank)
    other_rows = pl.ds(pl.multiple_of((1 - sides[0]) * rank, rank), rank)
    node = w_v[0].reshape(2 * rank, 2 * rank)

    def first(c):
        x0[c].wait_recv()
        stack[c, mine_rows, :] = p0_s[c]
        stack[c, other_rows, :] = p0_r[c]
        both = mm(node, stack[c]).astype(BF)
        stack[c] = both
        a_cat[c, pl.ds(0, rank), :] = stack[c, mine_rows, :]
        p1f[c] = p1f[c] - mm(g_v[0], both)
        p2f[c, :, keep] = p2f[c, :, keep] - mm(g_v[1], stack[c, :, keep])

    z1 = []

    def second_sum(c):
        x1[c].wait_recv()
        s1_s[c] = (p1f[c] + p1_r[c].astype(F32)).astype(BF)
        z1.append(send(s1_s.at[c], s1_r.at[c], near))

    def second(c):
        z1[c].wait_recv()
        a1 = (mm(weight(1, False), s1_s[c]) + mm(weight(1, True), s1_r[c])).astype(BF)
        a_cat[c, pl.ds(rank, rank), :] = a1
        a1 = a_cat[c, pl.ds(rank, rank), keep]
        p2f[c, :, keep] = (
            p2f[c, :, keep] - mm(g_v[2, :, pl.ds(0, rank)], a1) - mm(g_v[2, :, pl.ds(rank, rank)], a1)
        )

    n1 = []

    def third_sum(c):
        x2[c].wait_recv()
        p2f[c, :, keep] = p2f[c, :, keep] + p2_r[c].astype(F32)
        if c % 2 == 1:
            j = c // 2
            s2_s[j] = p2f[2 * j + 1 - sides[1], :, keep].astype(BF)
            n1.append(send(s2_s.at[j], s2_r.at[j], near))

    f1 = []

    def third_far(j):
        n1[j].wait_recv()
        t2_s[j] = (p2f[2 * j + sides[1], :, keep] + s2_r[j].astype(F32)).astype(BF)
        f1.append(send(t2_s.at[j], t2_r.at[j], far))

    n2 = []

    def third(j):
        f1[j].wait_recv()
        mine = 2 * j + sides[1]
        where = pl.ds(2 * rank, rank)
        a_cat[mine, where, keep] = (
            mm(weight(2, False), t2_s[j]) + mm(weight(2, True), t2_r[j])
        ).astype(BF)
        spot = a_cat.at[mine, where, keep]
        n2.append([send(spot, spot, to) for to in (diag, sib, near)])

    relay = []

    def relay_piece(k):
        a_across[k].wait_recv()
        where = piece_rows(flip(r, 2), k)
        relay.append(send(a_v.at[where, :], a_v.at[where, :], mate))

    def finish(c):
        own = pl.ds(c * cw, cw)
        for n in range(4):
            band = pl.ds(n * (rows // 4), rows // 4)
            out_v[band, own] = (start[band, own].astype(F32) - mm(c_v[band, :], a_cat[c])).astype(BF)

    relay_w(1)
    relay_w(2)
    start_rows(flip(r, 1))
    for c in range(CHUNKS):
        first(c)
    for c in range(CHUNKS):
        second_sum(c)
        if c == 1:
            w_relay[1].wait_recv()
            w_relay[2].wait_recv()
    second(0)
    second(1)
    third_sum(0)
    third_sum(1)
    for c in range(2, CHUNKS):
        second(c)
        third_sum(c)
    third_far(0)
    for k in range(pieces):
        relay_piece(k)
    for j in range(1, CHUNKS // 2):
        third_far(j)
    start_rows(flip(r, 2))
    for copy in relay:
        copy.wait_recv()
    start_rows(flip(flip(r, 2), 1))
    for j in range(CHUNKS // 2):
        third(j)
    for j in range(CHUNKS // 2):
        for copy in n2[j]:
            copy.wait_recv()
        finish(2 * j)
        finish(2 * j + 1)
    for copy in copies:
        copy.wait_send()


def local(right_sides, leaf_inverse, project_factors, correct_factors, *couplings):
    rows, cols = right_sides.shape
    blk, depth = leaf_inverse.shape
    levels, _, rank = project_factors.shape
    parts = lax.axis_size("rhs")
    cw = cols // CHUNKS
    full = lambda dtype: pltpu.VMEM((CHUNKS, rank, cw), dtype)
    thin = lambda dtype: pltpu.VMEM((CHUNKS, rank, cw // 2), dtype)
    part = lambda dtype: pltpu.VMEM((CHUNKS // 2, rank, cw // 2), dtype)
    copies = 96
    any_spec = pl.BlockSpec(memory_space=pltpu.HBM)
    return pl.pallas_call(
        kernel,
        out_shape=jax.ShapeDtypeStruct((rows, cols), BF),
        in_specs=[any_spec] * 7,
        out_specs=pl.BlockSpec(memory_space=pltpu.VMEM),
        scratch_shapes=[
            pltpu.VMEM((rows, cols), BF),
            pltpu.VMEM((rows, depth), BF),
            pltpu.VMEM((rows, levels * rank), BF),
            pltpu.VMEM((levels, rank, rows), BF),
            pltpu.VMEM((rows, levels * rank), BF),
            pltpu.VMEM((levels, parts) + couplings[0].shape[1:], BF),
            pltpu.VMEM((3, rank, 2 * rank), BF),
            pltpu.VMEM((levels, rank, depth // 2), F32),
            pltpu.VMEM((levels, rank, depth // 2), BF),
            pltpu.VMEM((levels, rank, depth // 2), BF),
            pltpu.VMEM((levels, 2, rank, depth // 2), BF),
            pltpu.VMEM((CHUNKS, 2 * rank, cw), BF),
            full(F32), full(BF), full(BF), full(F32), full(BF), full(BF), full(BF), full(BF),
            full(F32), thin(BF), thin(BF),
            part(BF), part(BF), part(BF), part(BF),
            pltpu.VMEM((CHUNKS, levels * rank, cw), BF),
            pltpu.VMEM((rows, cols), BF),
            pltpu.SemaphoreType.DMA((16,)),
            pltpu.SemaphoreType.DMA((copies,)),
            pltpu.SemaphoreType.DMA((copies,)),
        ],
        compiler_params=pltpu.CompilerParams(
            collective_id=0, has_side_effects=True, vmem_limit_bytes=48 * 1024 * 1024
        ),
    )(*(
        pltpu.with_memory_space_constraint(x, pltpu.HBM)
        for x in (right_sides, leaf_inverse, project_factors, correct_factors, *couplings)
    ))


def solution(mesh):
    in_specs = (
        P("leaf", "rhs"),
        P(("leaf", "rhs"), None),
        P(None, "leaf", None),
        P(None, "leaf", None),
        P(None, "rhs", None),
        P(None, "rhs", None),
        P(None, "rhs", None),
    )
    out_specs = P("leaf", "rhs")
    return jax.shard_map(local, mesh=mesh, in_specs=in_specs, out_specs=out_specs, check_vma=False)
```
